16 devices in a mesh: dp: 2 (over z), tp: 8 (over y, x, core).
Axes of the slice: x: 2, y: 2, z: 2, core: 2. Of those that a mesh axis runs over, the one named last changes fastest.
Arguments:
- x_in: bfloat16 [4096, 2048], P(('dp', 'tp')), parts along dimension 0
- grad_y: bfloat16 [4096, 2048], P(('dp', 'tp')), parts along dimension 0
- norm_gain: float32 [3, 2048], replicated
- w_qkv: bfloat16 [3, 2048, 6144], P(None, None, 'tp')
- w_out: bfloat16 [3, 2048, 2048], P(None, 'tp')
- w_gate: bfloat16 [3, 2048, 8192], P(None, None, 'tp')
- w_up: bfloat16 [3, 2048, 8192], P(None, None, 'tp')
- w_down: bfloat16 [3, 8192, 2048], P(None, 'tp')
Outputs:
- output 1: bfloat16 [4096, 2048], P(('dp', 'tp')), parts along dimension 0
- output 2: float32 [6, 2048], P('dp'), parts along dimension 0
- output 3: bfloat16 [6, 2048, 6144], P('dp', None, 'tp'), parts along dimension 0
- output 4: bfloat16 [6, 2048, 2048], P('dp', 'tp'), parts along dimension 0
- output 5: bfloat16 [6, 2048, 8192], P('dp', None, 'tp'), parts along dimension 0
- output 6: bfloat16 [6, 2048, 8192], P('dp', None, 'tp'), parts along dimension 0
- output 7: bfloat16 [6, 8192, 2048], P('dp', 'tp'), parts along dimension 0
There are 2 independent parts. The reference program is written for one: setup_inputs(seed, part) draws one part's arguments, and reference() takes and returns one part's arrays. A program takes and returns all parts, laid end to end along the dimension named above; an argument that names none is the same for every part.
All inputs are finite; a program needn't handle non-finite values.
Results may differ from the reference program's by a relative error of at most 0.02.
Values are sent between devices in bfloat16 or wider.
A program may use at most 1 GiB of HBM per device.

```python
import jax
import jax.numpy as jnp
from jax import lax

SEQ_LEN = 2048
D_MODEL = 2048
D_FF = 8192
HEADS = 16
KV_HEADS = 16
HEAD_DIM = 128
LAYERS = 3

GROUP_SIZE = HEADS // KV_HEADS
QKV_COLS = (HEADS + 2 * KV_HEADS) * HEAD_DIM
NORM_EPS = 1e-5
ROPE_BASE = 10000.0


def setup_inputs(seed: int = 0, part: int = 0) -> dict:
    data_keys = jax.random.split(jax.random.fold_in(jax.random.key(seed), part), 2)
    weight_keys = jax.random.split(jax.random.key(seed + 1), 6)
    x_in = jax.random.normal(data_keys[0], (SEQ_LEN, D_MODEL), jnp.float32)
    grad_y = jax.random.normal(data_keys[1], (SEQ_LEN, D_MODEL), jnp.float32)
    norm_gain = 1.0 + 0.3 * jax.random.normal(weight_keys[0], (LAYERS, D_MODEL), jnp.float32)
    w_qkv = jax.random.normal(weight_keys[1], (LAYERS, D_MODEL, QKV_COLS), jnp.float32) * D_MODEL ** -0.5
    w_out = jax.random.normal(weight_keys[2], (LAYERS, HEADS * HEAD_DIM, D_MODEL), jnp.float32) * (HEADS * HEAD_DIM) ** -0.5
    w_gate = jax.random.normal(weight_keys[3], (LAYERS, D_MODEL, D_FF), jnp.float32) * D_MODEL ** -0.5
    w_up = jax.random.normal(weight_keys[4], (LAYERS, D_MODEL, D_FF), jnp.float32) * D_MODEL ** -0.5
    w_down = jax.random.normal(weight_keys[5], (LAYERS, D_FF, D_MODEL), jnp.float32) * D_FF ** -0.5
    return {'x_in': x_in.astype(jnp.bfloat16), 'grad_y': grad_y.astype(jnp.bfloat16), 'norm_gain': norm_gain, 'w_qkv': w_qkv.astype(jnp.bfloat16), 'w_out': w_out.astype(jnp.bfloat16), 'w_gate': w_gate.astype(jnp.bfloat16), 'w_up': w_up.astype(jnp.bfloat16), 'w_down': w_down.astype(jnp.bfloat16)}


def rope_tables():
    half_dim = HEAD_DIM // 2
    freqs = ROPE_BASE ** (-2.0 * jnp.arange(half_dim, dtype=jnp.float32) / HEAD_DIM)
    angles = jnp.arange(SEQ_LEN, dtype=jnp.float32)[:, None] * freqs[None, :]
    return jnp.cos(angles)[:, None, None, :], jnp.sin(angles)[:, None, None, :]


def rotate(values, cos_tab, sin_tab):
    half_dim = values.shape[-1] // 2
    lower_half = values[..., :half_dim]
    upper_half = values[..., half_dim:]
    return jnp.concatenate([lower_half * cos_tab - upper_half * sin_tab, upper_half * cos_tab + lower_half * sin_tab], axis=-1)


def rms_scale(x_f32, gain_row):
    inv_rms = lax.rsqrt(jnp.mean(x_f32 * x_f32, axis=-1, keepdims=True) + NORM_EPS)
    return x_f32 * inv_rms * gain_row


def group_attention(operands):
    query, keys_rot, values_v = operands
    causal = jnp.arange(SEQ_LEN)[:, None] >= jnp.arange(SEQ_LEN)[None, :]
    scores = jnp.einsum('sgd,td->gst', query.astype(jnp.float32), keys_rot.astype(jnp.float32)) * HEAD_DIM ** -0.5
    attn_prob = jax.nn.softmax(jnp.where(causal, scores, -1e30), axis=-1).astype(jnp.bfloat16)
    return jnp.einsum('gst,td->sgd', attn_prob.astype(jnp.float32), values_v.astype(jnp.float32)).astype(jnp.bfloat16)


def decoder_block(x_cur, gain_row, w_qkv_l, w_out_l, w_gate_l, w_up_l, w_down_l, cos_tab, sin_tab):
    x_f32 = x_cur.astype(jnp.float32)
    normed = rms_scale(x_f32, gain_row).astype(jnp.bfloat16).astype(jnp.float32)
    qkv_all = jnp.dot(normed, w_qkv_l.astype(jnp.float32), preferred_element_type=jnp.float32).astype(jnp.bfloat16)
    qkv_all = qkv_all.reshape(SEQ_LEN, KV_HEADS, GROUP_SIZE + 2, HEAD_DIM)
    rotated = rotate(qkv_all[:, :, :GROUP_SIZE + 1].astype(jnp.float32), cos_tab, sin_tab).astype(jnp.bfloat16)
    operands = (jnp.moveaxis(rotated[:, :, :GROUP_SIZE], 1, 0), jnp.moveaxis(rotated[:, :, GROUP_SIZE], 1, 0), jnp.moveaxis(qkv_all[:, :, GROUP_SIZE + 1], 1, 0))
    attn_out = lax.map(jax.checkpoint(group_attention), operands)
    attn_out = jnp.moveaxis(attn_out, 0, 1).reshape(SEQ_LEN, HEADS * HEAD_DIM)
    gate_act = jnp.dot(normed, w_gate_l.astype(jnp.float32), preferred_element_type=jnp.float32).astype(jnp.bfloat16)
    up_act = jnp.dot(normed, w_up_l.astype(jnp.float32), preferred_element_type=jnp.float32).astype(jnp.bfloat16)
    hidden = (jax.nn.silu(gate_act.astype(jnp.float32)) * up_act.astype(jnp.float32)).astype(jnp.bfloat16)
    block_sum = x_f32 + jnp.dot(attn_out.astype(jnp.float32), w_out_l.astype(jnp.float32), preferred_element_type=jnp.float32) + jnp.dot(hidden.astype(jnp.float32), w_down_l.astype(jnp.float32), preferred_element_type=jnp.float32)
    return block_sum.astype(jnp.bfloat16)


def stack_forward(x_in, norm_gain, w_qkv, w_out, w_gate, w_up, w_down):
    cos_tab, sin_tab = rope_tables()

    def body(x_cur, layer_weights):
        gain_row, w_qkv_l, w_out_l, w_gate_l, w_up_l, w_down_l = layer_weights
        return decoder_block(x_cur, gain_row, w_qkv_l, w_out_l, w_gate_l, w_up_l, w_down_l, cos_tab, sin_tab), None

    return lax.scan(body, x_in, (norm_gain, w_qkv, w_out, w_gate, w_up, w_down))[0]


def reference(x_in, grad_y, norm_gain, w_qkv, w_out, w_gate, w_up, w_down):
    pullback = jax.vjp(stack_forward, x_in, norm_gain, w_qkv, w_out, w_gate, w_up, w_down)[1]
    grad_x, grad_gain, grad_qkv, grad_out, grad_gate, grad_up, grad_down = pullback(grad_y)
    return (grad_x, grad_gain, grad_qkv, grad_out, grad_gate, grad_up, grad_down)
```

```python
import functools
import jax
import jax.numpy as jnp
from jax import lax
from jax.experimental import pallas as pl
from jax.experimental.pallas import tpu as pltpu
from jax.sharding import PartitionSpec as P

HEAD_DIM = 128
NORM_EPS = 1e-5
ROPE_BASE = 10000.0
SCALE = HEAD_DIM ** -0.5
QB = 256
NT = (((1,), (1,)), ((), ()))
NN = (((1,), (0,)), ((), ()))
F32 = jnp.float32
BF16 = jnp.bfloat16


def call(kernel, ins, in_specs, after=(), n_out=1, **kw):
    n_in, n_tok = len(ins), len(after)

    def body(*refs):
        kernel(*refs[:n_in], *refs[n_in + n_tok:])

    specs = list(in_specs) + [pl.BlockSpec(memory_space=pl.ANY)] * n_tok
    return pl.pallas_call(body if n_tok else kernel, in_specs=specs, **kw)(*ins, *after)


def dot(a, b, dims=NN):
    return lax.dot_general(a, b, dims, preferred_element_type=F32)


def rms_scale(x_f32, gain_row):
    inv_rms = lax.rsqrt(jnp.mean(x_f32 * x_f32, axis=-1, keepdims=True) + NORM_EPS)
    return x_f32 * inv_rms * gain_row


def gated(gate_f32, up_f32):
    return jax.nn.silu(gate_f32) * up_f32


def rope_tables(seq_len):
    half_dim = HEAD_DIM // 2
    freqs = ROPE_BASE ** (-2.0 * jnp.arange(half_dim, dtype=F32) / HEAD_DIM)
    angles = jnp.arange(seq_len, dtype=F32)[:, None] * freqs[None, :]
    cos, sin = jnp.cos(angles), jnp.sin(angles)
    return jnp.concatenate([cos, cos], axis=1), jnp.concatenate([-sin, sin], axis=1)


def diag_mask(s, fill):
    r = lax.broadcasted_iota(jnp.int32, s.shape, 0)
    c = lax.broadcasted_iota(jnp.int32, s.shape, 1)
    return jnp.where(c >= r, s, fill)


def attn_fwd_kernel(n_prev, n_blk, perm, qkv, *refs):
    if n_prev:
        prev, cos, sin, rot, o, lse, s_scr, vt_scr = refs
    else:
        cos, sin, rot, o, lse, s_scr, vt_scr = refs
    rows = qkv.shape[0]
    blk = rows // n_blk
    for k in range(n_blk):
        j = pl.multiple_of(perm[0, k] * blk, blk)
        x = qkv[k * blk:(k + 1) * blk, :]
        c = cos[pl.ds(j, blk), :]
        s = sin[pl.ds(j, blk), :]
        for part in range(2):
            v = x[:, part * 128:(part + 1) * 128].astype(F32)
            rot[pl.ds(j, blk), part * 128:(part + 1) * 128] = (v * c + pltpu.roll(v, 64, 1) * s).astype(BF16)
        rot[pl.ds(j, blk), 256:384] = x[:, 256:384]
    srcs = []
    if n_prev:
        srcs += [(prev, b) for b in range(n_prev)]
    srcs += [(rot, b) for b in range(rows // QB)]
    for n, (ref, b) in enumerate(srcs):
        vt_scr[:, n * QB:(n + 1) * QB] = ref[b * QB:(b + 1) * QB, 256:384].astype(F32).T.astype(BF16)
    for i in range(rows // QB):
        q = rot[i * QB:(i + 1) * QB, 0:128]
        n_kv = n_prev + i + 1
        m = None
        for n in range(n_kv):
            ref, b = srcs[n]
            s = dot(ref[b * QB:(b + 1) * QB, 128:256], q, NT) * SCALE
            if n == n_kv - 1:
                s = diag_mask(s, -1e30)
            s_scr[n * QB:(n + 1) * QB, :] = s
            bm = jnp.max(s, axis=0, keepdims=True)
            m = bm if m is None else jnp.maximum(m, bm)
        l = jnp.zeros((1, QB), F32)
        ot = jnp.zeros((128, QB), F32)
        for n in range(n_kv):
            p = jnp.exp(s_scr[n * QB:(n + 1) * QB, :] - m)
            l = l + jnp.sum(p, axis=0, keepdims=True)
            ot = ot + dot(vt_scr[:, n * QB:(n + 1) * QB], p.astype(BF16))
        out = (ot / l).T.astype(BF16)
        for t in range(QB // blk):
            r = pl.multiple_of(perm[1, i * (QB // blk) + t] * blk, blk)
            o[pl.ds(r, blk), :] = out[t * blk:(t + 1) * blk, :]
        lse[0, :, i * QB:(i + 1) * QB] = m + jnp.log(l)


def attn_fwd(perm, qkv, prev, cos, sin, after=()):
    rows, cols = qkv.shape
    heads = cols // 384
    n_prev = 0 if prev is None else prev.shape[0] // QB
    head_spec = pl.BlockSpec((rows, 384), lambda h: (0, h))
    tab_spec = pl.BlockSpec((rows, 128), lambda h: (0, 0))
    ins = [perm, qkv] + ([prev] if n_prev else []) + [cos, sin]
    specs = [pl.BlockSpec(memory_space=pltpu.SMEM), head_spec] + ([pl.BlockSpec((prev.shape[0], 384), lambda h: (0, h))] if n_prev else []) + [tab_spec, tab_spec]
    n_kv = n_prev * QB + rows
    return call(
        functools.partial(attn_fwd_kernel, n_prev, perm.shape[1]), ins, specs, after,
        grid=(heads,),
        out_specs=[head_spec, pl.BlockSpec((rows, 128), lambda h: (0, h)), pl.BlockSpec((1, 1, rows), lambda h: (h, 0, 0))],
        out_shape=[jax.ShapeDtypeStruct((rows, cols), BF16), jax.ShapeDtypeStruct((rows, heads * 128), BF16), jax.ShapeDtypeStruct((heads, 1, rows), F32)],
        scratch_shapes=[pltpu.VMEM((n_kv, QB), F32), pltpu.VMEM((128, n_kv), BF16)],
        cost_estimate=pl.CostEstimate(flops=8 * heads * rows * n_kv * 128, bytes_accessed=6 * rows * cols, transcendentals=heads * rows * n_kv),
    )


def attn_bwd_kernel(n_prev, has_in, n_blk, perm, rot, *refs):
    refs = list(refs)
    prev = refs.pop(0) if n_prev else None
    o, do, lse = refs[:3]
    refs = refs[3:]
    dkv_in = refs.pop(0) if has_in else None
    cos, sin, dqkv = refs[:3]
    refs = refs[3:]
    dkv_out = refs.pop(0) if n_prev else None
    kt_scr, dk_scr, dv_scr = refs
    rows = rot.shape[0]
    blk = rows // n_blk
    srcs = []
    if n_prev:
        srcs += [(prev, b) for b in range(n_prev)]
    srcs += [(rot, b) for b in range(rows // QB)]
    for n, (ref, b) in enumerate(srcs):
        kt_scr[:, n * QB:(n + 1) * QB] = ref[b * QB:(b + 1) * QB, 128:256].astype(F32).T.astype(BF16)
    if has_in:
        dk_scr[...] = dkv_in[0, :, 0:128]
        dv_scr[...] = dkv_in[0, :, 128:256]
    else:
        dk_scr[...] = jnp.zeros_like(dk_scr)
        dv_scr[...] = jnp.zeros_like(dv_scr)

    def unrotate(v, j):
        c = cos[pl.ds(j, blk), :]
        s = sin[pl.ds(j, blk), :]
        return (v * c - pltpu.roll(v, 64, 1) * s).astype(BF16)

    for i in range(rows // QB):
        q = rot[i * QB:(i + 1) * QB, 0:128]
        rel = [pl.multiple_of(perm[1, i * (QB // blk) + t] * blk, blk) for t in range(QB // blk)]
        d_o = jnp.concatenate([do[pl.ds(r, blk), :] for r in rel], axis=0)
        o_b = jnp.concatenate([o[pl.ds(r, blk), :] for r in rel], axis=0)
        delta = jnp.sum((d_o.astype(F32) * o_b.astype(F32)).T, axis=0, keepdims=True)
        ls = lse[0, :, i * QB:(i + 1) * QB]
        n_kv = n_prev + i + 1
        dqt = jnp.zeros((128, QB), F32)
        for n in range(n_kv):
            ref, b = srcs[n]
            sl = slice(n * QB, (n + 1) * QB)
            s = dot(ref[b * QB:(b + 1) * QB, 128:256], q, NT) * SCALE
            if n == n_kv - 1:
                s = diag_mask(s, -1e30)
            p = jnp.exp(s - ls)
            dp = dot(ref[b * QB:(b + 1) * QB, 256:384], d_o, NT).astype(BF16).astype(F32)
            dv_scr[sl, :] += dot(p.astype(BF16), d_o)
            ds = (p * (dp - delta) * SCALE).astype(BF16)
            dk_scr[sl, :] += dot(ds, q)
            dqt = dqt + dot(kt_scr[:, sl], ds)
        dq = dqt.T.astype(BF16).astype(F32)
        for t, r in enumerate(rel):
            j = i * QB + t * blk
            dqkv[pl.ds(r, blk), 0:128] = unrotate(dq[t * blk:(t + 1) * blk, :], j)
    base = n_prev * QB
    for k in range(n_blk):
        r = pl.multiple_of(perm[1, k] * blk, blk)
        sl = slice(base + k * blk, base + (k + 1) * blk)
        dqkv[pl.ds(r, blk), 128:256] = unrotate(dk_scr[sl, :].astype(BF16).astype(F32), k * blk)
        dqkv[pl.ds(r, blk), 256:384] = dv_scr[sl, :].astype(BF16)
    if n_prev:
        dkv_out[0, :, 0:128] = dk_scr[0:base, :]
        dkv_out[0, :, 128:256] = dv_scr[0:base, :]


def attn_bwd(perm, rot, prev, o, do, lse, dkv_in, cos, sin, after=()):
    rows, cols = rot.shape
    heads = cols // 384
    n_prev = 0 if prev is None else prev.shape[0] // QB
    head_spec = pl.BlockSpec((rows, 384), lambda h: (0, h))
    o_spec = pl.BlockSpec((rows, 128), lambda h: (0, h))
    tab_spec = pl.BlockSpec((rows, 128), lambda h: (0, 0))
    ins, specs = [perm, rot], [pl.BlockSpec(memory_space=pltpu.SMEM), head_spec]
    if n_prev:
        ins.append(prev)
        specs.append(pl.BlockSpec((prev.shape[0], 384), lambda h: (0, h)))
    ins += [o, do, lse]
    specs += [o_spec, o_spec, pl.BlockSpec((1, 1, rows), lambda h: (h, 0, 0))]
    if dkv_in is not None:
        ins.append(dkv_in)
        specs.append(pl.BlockSpec((1, rows, 256), lambda h: (h, 0, 0)))
    ins += [cos, sin]
    specs += [tab_spec, tab_spec]
    outs, ospecs = [jax.ShapeDtypeStruct((rows, cols), BF16)], [head_spec]
    n_kv = n_prev * QB + rows
    if n_prev:
        outs.append(jax.ShapeDtypeStruct((heads, n_prev * QB, 256), F32))
        ospecs.append(pl.BlockSpec((1, n_prev * QB, 256), lambda h: (h, 0, 0)))
    return call(
        functools.partial(attn_bwd_kernel, n_prev, dkv_in is not None, perm.shape[1]), ins, specs, after,
        grid=(heads,), out_specs=ospecs, out_shape=outs,
        scratch_shapes=[pltpu.VMEM((128, n_kv), BF16), pltpu.VMEM((n_kv, 128), F32), pltpu.VMEM((n_kv, 128), F32)],
        cost_estimate=pl.CostEstimate(flops=16 * heads * rows * n_kv * 128, bytes_accessed=8 * rows * cols, transcendentals=heads * rows * n_kv),
    )
def whole(shape):
    return pl.BlockSpec(shape, lambda *_: (0,) * len(shape))


def gemm_cost(flops, *arrays):
    return pl.CostEstimate(flops=flops, bytes_accessed=sum(a.size * a.dtype.itemsize for a in arrays), transcendentals=0)


def qkv_kernel(u, w, out):
    out[...] = dot(u[...], w[0]).astype(BF16)


def qkv_proj(u, w, l, after=(), bn=256):
    m, d = u.shape
    n = w.shape[2]
    return call(
        qkv_kernel, [u, w], [whole((m, d)), pl.BlockSpec((1, d, bn), lambda j: (l, 0, j))], after,
        grid=(n // bn,),
        out_specs=pl.BlockSpec((m, bn), lambda j: (0, j)),
        out_shape=jax.ShapeDtypeStruct((m, n), BF16),
        cost_estimate=gemm_cost(2 * m * d * n, u, u),
    )


def mlp_fwd_kernel(u, wg, wu, a, b, *h):
    uv = u[...]
    av = dot(uv, wg[0]).astype(BF16)
    bv = dot(uv, wu[0]).astype(BF16)
    a[...] = av
    b[...] = bv
    if h:
        h[0][...] = gated(av.astype(F32), bv.astype(F32)).astype(BF16)


def mlp_fwd(u, wg, wu, l, with_hidden, after=(), bn=256):
    m, d = u.shape
    n = wg.shape[2]
    w_spec = pl.BlockSpec((1, d, bn), lambda j: (l, 0, j))
    o_spec = pl.BlockSpec((m, bn), lambda j: (0, j))
    n_out = 3 if with_hidden else 2
    return call(
        mlp_fwd_kernel, [u, wg, wu], [whole((m, d)), w_spec, w_spec], after,
        grid=(n // bn,), out_specs=[o_spec] * n_out,
        out_shape=[jax.ShapeDtypeStruct((m, n), BF16)] * n_out,
        cost_estimate=gemm_cost(4 * m * d * n, u, u, u),
    )


def position(me, flip_core, flip_x, flip_y):
    core, x, y = me % 2, (me // 2) % 2, me // 4
    core = 1 - core if flip_core else core
    x = 1 - x if flip_x else x
    y = 1 - y if flip_y else y
    return y * 4 + x * 2 + core


def pair_sum_kernel(n_pairs, dims, blk, *refs):
    lhs, rhs = refs[:n_pairs], refs[n_pairs:2 * n_pairs]
    keep_a, send_a, keep_b, send_b, own, sent, got, send_sem, recv_sem = refs[2 * n_pairs:]
    j = pl.program_id(0)
    nb = got.shape[0]
    me = lax.axis_index('tp')
    peer = position(me, True, False, False)

    @pl.when(j == 0)
    def _():
        barrier = pltpu.get_barrier_semaphore()
        pl.semaphore_signal(barrier, inc=1, device_id={'tp': peer}, device_id_type=pl.DeviceIdType.MESH)
        pl.semaphore_wait(barrier, 1)

    def copy(b):
        return pltpu.make_async_remote_copy(
            src_ref=sent.at[b], dst_ref=got.at[b], send_sem=send_sem.at[b], recv_sem=recv_sem.at[b],
            device_id={'tp': peer}, device_id_type=pl.DeviceIdType.MESH)

    def product(flip_core, x_major):
        acc = None
        order = [(a, b) if x_major else (b, a) for a in (0, 1) for b in (0, 1)]
        offs = [pl.multiple_of(position(me, flip_core, fx, fy) * blk, blk) for fx, fy in order]
        for a, w in zip(lhs, rhs):
            rows = jnp.concatenate([a[pl.ds(r, blk), :] for r in offs], axis=0)
            t = dot(rows, w[0], dims)
            acc = t if acc is None else acc + t
        return acc

    for x_major, cond in ((True, j < nb // 2), (False, jnp.logical_and(j >= nb // 2, j < nb))):
        @pl.when(cond)
        def _():
            sent[j] = product(True, x_major)
            copy(j).start()
            own[j % 2] = product(False, x_major)

    for keep, send, cond in ((keep_a, send_a, jnp.logical_and(j >= 1, j <= nb // 2)), (keep_b, send_b, j > nb // 2)):
        @pl.when(cond)
        def _():
            copy(j - 1).wait_recv()
            total = own[(j - 1) % 2] + got[j - 1]
            keep[...] = total[:2 * blk]
            send[...] = total[2 * blk:]

    @pl.when(j == nb)
    def _():
        for b in range(nb):
            copy(b).wait_send()


def pair_sum(lhs, weights, l, nt, cid, after=(), bn=512):
    m = lhs[0].shape[0]
    blk = m // 8
    n = weights[0].shape[1] if nt else weights[0].shape[2]
    nb = n // bn
    specs = [whole(a.shape) for a in lhs]
    if nt:
        specs += [pl.BlockSpec((1, bn, w.shape[2]), lambda j: (l, jnp.minimum(j, nb - 1), 0)) for w in weights]
    else:
        specs += [pl.BlockSpec((1, w.shape[1], bn), lambda j: (l, 0, jnp.minimum(j, nb - 1))) for w in weights]
    top = nb // 2 - 1
    a_spec = pl.BlockSpec((2 * blk, bn), lambda j: (0, jnp.minimum(jnp.maximum(j - 1, 0), top)))
    b_spec = pl.BlockSpec((2 * blk, bn), lambda j: (0, jnp.minimum(jnp.maximum(j - 1 - nb // 2, 0), top)))
    k = sum(a.shape[1] for a in lhs)
    return call(
        functools.partial(pair_sum_kernel, len(lhs), NT if nt else NN, blk), list(lhs) + list(weights), specs, after,
        grid=(nb + 1,), out_specs=[a_spec, a_spec, b_spec, b_spec],
        out_shape=[jax.ShapeDtypeStruct((2 * blk, n // 2), F32)] * 4,
        scratch_shapes=[pltpu.VMEM((2, m // 2, bn), F32), pltpu.VMEM((nb, m // 2, bn), F32), pltpu.VMEM((nb, m // 2, bn), F32),
                        pltpu.SemaphoreType.DMA((nb,)), pltpu.SemaphoreType.DMA((nb,))],
        compiler_params=pltpu.CompilerParams(collective_id=cid, has_side_effects=True),
        cost_estimate=gemm_cost(2 * m * n * k, *lhs),
    )


def mlp_bwd_kernel(dy, wd, wo, a, b, dattn, dg, du, h):
    dyv = dy[...]

    @pl.when(pl.program_id(0) == 0)
    def _():
        dattn[...] = dot(dyv, wo[0], NT).astype(BF16)

    dh = dot(dyv, wd[0], NT).astype(BF16).astype(F32)
    gate = a[...].astype(F32)
    up = b[...].astype(F32)
    sig = jax.nn.sigmoid(gate)
    silu = gate * sig
    h[...] = (silu * up).astype(BF16)
    du[...] = (dh * silu).astype(BF16)
    dg[...] = (dh * up * (sig * (1.0 + gate * (1.0 - sig)))).astype(BF16)


def mlp_bwd(dy, wd, wo, a, b, l, after=(), bn=256):
    m, d = dy.shape
    n, k = wd.shape[1], wo.shape[1]
    col = pl.BlockSpec((m, bn), lambda j: (0, j))
    return call(
        mlp_bwd_kernel, [dy, wd, wo, a, b],
        [whole((m, d)), pl.BlockSpec((1, bn, d), lambda j: (l, j, 0)), pl.BlockSpec((1, k, d), lambda j: (l, 0, 0)), col, col], after,
        grid=(n // bn,),
        out_specs=[whole((m, k)), col, col, col],
        out_shape=[jax.ShapeDtypeStruct((m, k), BF16)] + [jax.ShapeDtypeStruct((m, n), BF16)] * 3,
        cost_estimate=gemm_cost(2 * m * d * (n + k), dy, a, a, a, a),
    )


TN = (((0,), (0,)), ((), ()))


def wgrad_kernel(n, *refs):
    acc = dot(refs[0][...], refs[n][...], TN)
    for a, b in zip(refs[1:n], refs[n + 1:2 * n]):
        acc = acc + dot(a[...], b[...], TN)
    refs[-1][0] = acc.astype(BF16)


def wgrad(lhs, rhs, l, layers, buf, after=(), bm=256):
    k, m = lhs[0].shape
    n = rhs[0].shape[1]
    specs = [pl.BlockSpec((k, bm), lambda i: (0, i))] * len(lhs) + [whole((k, n))] * len(rhs)
    ins = list(lhs) + list(rhs)
    alias = {}
    if buf is not None:
        alias = {len(ins): 0}
        ins.append(buf)
        specs.append(pl.BlockSpec(memory_space=pl.ANY))
    return call(
        functools.partial(wgrad_kernel, len(lhs)), ins, specs, after,
        grid=(m // bm,), out_specs=pl.BlockSpec((1, bm, n), lambda i: (l, i, 0)),
        out_shape=jax.ShapeDtypeStruct((layers, m, n), BF16), input_output_aliases=alias,
        cost_estimate=gemm_cost(2 * m * n * k * len(lhs), *lhs, *rhs),
    )


def xor_perm(n, bit):
    return [(i, i ^ bit) for i in range(n)]


def swap(v, bit):
    return lax.ppermute(v, 'tp', xor_perm(8, bit))


def tree_sum(v):
    for bit in (1, 2, 4):
        v = v + swap(v, bit)
    return v


def to_halves(x_loc):
    me = lax.axis_index('tp')
    top, bot = jnp.split(x_loc, 2, axis=0)
    first = me < 4
    half = 4
    pa = [(s, 2 * s) for s in range(half)] + [(half + s, 2 * s + 1) for s in range(half)]
    pb = [(s, 2 * s + 1) for s in range(half)] + [(half + s, 2 * s) for s in range(half)]
    ra = lax.ppermute(jnp.where(first, top, bot), 'tp', pa)
    rb = lax.ppermute(jnp.where(first, bot, top), 'tp', pb)
    even = me % 2 == 0
    return [jnp.where(even, ra, rb), jnp.where(even, rb, ra)]


def from_halves(c0, c1):
    me = lax.axis_index('tp')
    even = me % 2 == 0
    half = 4
    pa = [(2 * s, s) for s in range(half)] + [(2 * s + 1, half + s) for s in range(half)]
    pb = [(2 * s + 1, s) for s in range(half)] + [(2 * s, half + s) for s in range(half)]
    ra = lax.ppermute(jnp.where(even, c0, c1), 'tp', pa)
    rb = lax.ppermute(jnp.where(even, c1, c0), 'tp', pb)
    first = me < half
    return jnp.concatenate([jnp.where(first, ra, rb), jnp.where(first, rb, ra)], axis=0)


def scatter_first(parts):
    keep_a, send_a, keep_b, send_b = parts
    return keep_a + swap(send_a, 2), keep_b + swap(send_b, 4)


def scatter_second(a, b):
    r = a.shape[0] // 2
    return jnp.concatenate([a[:r] + swap(a[r:], 4), b[:r] + swap(b[r:], 2)], axis=-1)


def gather_rows(u):
    return lax.all_gather(u, 'tp', axis=0, tiled=True)


def solution(mesh):
    row_spec = P(('dp', 'tp'), None)
    col_spec = P(None, None, 'tp')
    inner_spec = P(None, 'tp', None)

    def device_program(x_loc, dy_loc, norm_gain, w_qkv, w_out, w_gate, w_up, w_down):
        n_layers = w_qkv.shape[0]
        seq = x_loc.shape[0] * mesh.shape['tp']
        cos, sin = rope_tables(seq)
        half = seq // 2
        tabs = [(cos[:half], sin[:half]), (cos[half:], sin[half:])]
        perm = jnp.tile(jnp.arange(8, dtype=jnp.int32)[None], (2, 1))
        xs = to_halves(x_loc)
        dys = to_halves(dy_loc)
        saved = {}
        tok, pend = (), None
        for l in range(n_layers):
            last = l == n_layers - 1
            prev = None
            for c in range(2):
                u = rms_scale(xs[c].astype(F32), norm_gain[l]).astype(BF16)
                u_full = gather_rows(u)
                qkv = qkv_proj(u_full, w_qkv, l, tok)
                rot, o, lse = attn_fwd(perm, qkv, prev, *tabs[c])
                acts = mlp_fwd(u_full, w_gate, w_up, l, not last, (o,))
                saved[l, c] = (xs[c], u, rot, o, lse, acts[0], acts[1])
                prev = rot
                tok = (acts[0],)
                mid = None
                if pend is not None:
                    pc, parts, px = pend
                    mid = scatter_first(parts)
                if not last:
                    parts = pair_sum([o, acts[2]], [w_out, w_down], l, False, 2 * l + c, mid or ())
                    tok = (parts[0],)
                if mid is not None:
                    xs[pc] = (px.astype(F32) + scatter_second(*mid)).astype(BF16)
                pend = None if last else (c, parts, xs[c])
        bufs = [None] * 5
        gains = [None] * n_layers
        us = [saved[n_layers - 1, c][1] for c in range(2)]
        us, dys = lax.optimization_barrier((us, dys))

        def finish(l, c, mid, x, dy):
            d_normed = scatter_second(*mid).astype(BF16)
            pull = jax.vjp(rms_scale, x.astype(F32), norm_gain[l])[1]
            d_x, d_gain = pull(d_normed.astype(F32))
            gains[l] = d_gain if gains[l] is None else gains[l] + d_gain
            return (dy.astype(F32) + d_x).astype(BF16)

        for l in reversed(range(n_layers)):
            s1, s0 = saved[l, 1], saved[l, 0]
            cid = 2 * n_layers + 2 * l
            dy1, dy0 = gather_rows(dys[1]), gather_rows(dys[0])
            da1, dg1, du1, h1 = mlp_bwd(dy1, w_down, w_out, s1[5], s1[6], l, tok)
            dqkv1, dkv = attn_bwd(perm, s1[2], s0[2], s1[3], da1, s1[4], None, *tabs[1])
            parts1 = pair_sum([dqkv1, dg1, du1], [w_qkv, w_gate, w_up], l, True, cid)
            da0, dg0, du0, h0 = mlp_bwd(dy0, w_down, w_out, s0[5], s0[6], l, (parts1[0],))
            dqkv0, = attn_bwd(perm, s0[2], None, s0[3], da0, s0[4], dkv, *tabs[0])
            mid1 = scatter_first(parts1)
            parts0 = pair_sum([dqkv0, dg0, du0], [w_qkv, w_gate, w_up], l, True, cid + 1, mid1)
            dys1 = finish(l, 1, mid1, s1[0], dys[1])
            uf = [gather_rows(v) for v in us]
            bufs[4] = wgrad([h0, h1], [dy0, dy1], l, n_layers, bufs[4], (parts0[0], dys1))
            bufs[1] = wgrad([s0[3], s1[3]], [dy0, dy1], l, n_layers, bufs[1], (bufs[4],))
            bufs[2] = wgrad(uf, [dg0, dg1], l, n_layers, bufs[2], (bufs[1],))
            mid0 = scatter_first(parts0)
            bufs[3] = wgrad(uf, [du0, du1], l, n_layers, bufs[3], (bufs[2], *mid0))
            dys0 = finish(l, 0, mid0, s0[0], dys[0])
            bufs[0] = wgrad(uf, [dqkv0, dqkv1], l, n_layers, bufs[0], (bufs[3], dys0))
            tok = (bufs[0],)
            dys = [dys0, dys1]
            if l:
                us = [saved[l - 1, c][1] for c in range(2)]
                us, bufs[0], bufs[2], bufs[3] = lax.optimization_barrier((us, bufs[0], bufs[2], bufs[3]))
        grad_gain = tree_sum(jnp.stack(gains))
        return (from_halves(dys[0], dys[1]), grad_gain, *bufs)

    return jax.shard_map(device_program, mesh=mesh, in_specs=(row_spec, row_spec, P(None, None), col_spec, inner_spec, col_spec, col_spec, inner_spec), out_specs=(row_spec, P('dp', None), P('dp', None, 'tp'), P('dp', 'tp', None), P('dp', None, 'tp'), P('dp', None, 'tp'), P('dp', 'tp', None)), check_vma=False)
```
